32 devices in a mesh: shard: 8 (over y, x, core), model: 4 (over z).
Axes of the slice: x: 2, y: 2, z: 4, core: 2. Of those that a mesh axis runs over, the one named last changes fastest.
Arguments:
- weight_gate: float32 [3072, 8192], P('shard', 'model'), may hold values from -0.15625 to 0.15625
- smooth_gate: float32 [3072, 8192], P('shard', 'model'), may hold values from -0.109375 to 0.109375
- weight_up: float32 [3072, 8192], P('shard', 'model'), may hold values from -0.15625 to 0.15625
- smooth_up: float32 [3072, 8192], P('shard', 'model'), may hold values from -0.109375 to 0.109375
- norm_train: float32 [3072], P(('shard', 'model')), may hold values from 0.25 to 1.75
- norm_step: float32 [3072], P(('shard', 'model')), may hold values from -0.3 to 0.3
Outputs:
- serving_gate: bfloat16 [3072, 8192], P(None, 'model')
- serving_up: bfloat16 [3072, 8192], P(None, 'model')
- factor_gate: float32 [8192], P('model')
- factor_up: float32 [8192], P('model')
- serve_norm: bfloat16 [3072], replicated
- whole_gate: float32 [3072, 8192], P('shard', 'model')
- whole_up: float32 [3072, 8192], P('shard', 'model')
The draws below stay inside these ranges and needn't reach their ends.
All inputs are finite; a program needn't handle non-finite values. Where the reference program divides by a largest or mean magnitude, that divisor is 1e-20 or more.
Results may differ from the reference program's by a relative error of at most 0.001.
Values may be sent and summed in bfloat16 or wider, within the bound.
A program may use at most 128 MiB of HBM per device.

```python
import jax
import jax.numpy as jnp

D_MODEL = 3072
D_INNER = 8192


def raised(result, key, source, target, blocks, factor):
    owner, partner = [(jnp.arange(result.shape[dim]) // (result.shape[dim] // blocks)).reshape([-1 if axis == dim else 1 for axis in range(result.ndim)]) for dim in (source, target)]
    chosen = jax.random.permutation(key, blocks)[partner]
    strong = (owner == chosen) | (owner == (partner + blocks // 2) % blocks)
    return jnp.where(strong, factor * result, result)


def block_levels(rng, extent, split, smallest, top_value):
    def one(dim, blocks):
        heights = jax.random.uniform(jax.random.fold_in(jax.random.fold_in(rng, 6), dim), (blocks,), jnp.float32, smallest / len(split), top_value / len(split))
        return jnp.repeat(jnp.exp(heights), extent[dim] // blocks).reshape((-1,) + (1,) * (len(extent) - dim - 1))

    level = one(*split[0])
    for cut in split[1:]:
        level = level * one(*cut)
    return level


def scatter_about(stream_key, dims, scale, most, pieces=(), kind=jnp.bfloat16):
    factor_of = block_levels(stream_key, dims, pieces, -0.22, 0.18) if pieces else 1.0
    values = jax.random.normal(stream_key, dims, jnp.float32) * scale * factor_of
    return jnp.minimum(jnp.maximum(values, -most), most).astype(kind)


def noise_with(key, dims, scale, limit, cuts, heavy, kind=jnp.bfloat16):
    values = scale * jax.random.normal(key, dims, jnp.float32)
    if cuts:
        values = values * block_levels(key, dims, cuts, -0.22, 0.18)
    return jnp.clip(raised(values, jax.random.fold_in(key, 3), *heavy), -limit, limit).astype(kind)


def setup_inputs(seed: int = 0) -> dict:
    arg_keys = jax.random.split(jax.random.key(seed), 7)
    return {
        "weight_gate": noise_with(arg_keys[0], (D_MODEL, D_INNER), D_MODEL ** -0.5, 0.15625, ((0, 8), (1, 4)), (0, 1, 8, 2.0), jnp.float32),
        "smooth_gate": scatter_about(arg_keys[1], (D_MODEL, D_INNER), D_MODEL ** -0.5, 0.109375, ((0, 8), (1, 4)), jnp.float32),
        "weight_up": noise_with(arg_keys[2], (D_MODEL, D_INNER), D_MODEL ** -0.5, 0.15625, ((0, 8), (1, 4)), (0, 1, 8, 2.0), jnp.float32),
        "smooth_up": scatter_about(arg_keys[3], (D_MODEL, D_INNER), D_MODEL ** -0.5, 0.109375, ((0, 8), (1, 4)), jnp.float32),
        "norm_train": jnp.clip(1.0 + 0.15 * jax.random.normal(arg_keys[4], (D_MODEL,), jnp.float32), 0.25, 1.75),
        "norm_step": jnp.clip(jax.random.uniform(arg_keys[5], (D_MODEL,), jnp.float32, -0.3, 0.3) * block_levels(arg_keys[5], (D_MODEL,), ((0, 32),), -0.4, 0.0), -0.3, 0.3),
    }


keep_rate = 0.7


def reference(weight_gate, smooth_gate, weight_up, smooth_up, norm_train, norm_step):
    whole_gate = keep_rate * smooth_gate + (1.0 - keep_rate) * weight_gate
    whole_up = keep_rate * smooth_up + (1.0 - keep_rate) * weight_up
    factor_gate = jnp.max(jnp.abs(whole_gate), axis=0)
    serving_gate = (whole_gate / factor_gate).astype(jnp.bfloat16)
    factor_up = jnp.max(jnp.abs(whole_up), axis=0)
    serving_up = (whole_up / factor_up).astype(jnp.bfloat16)
    serve_norm = (norm_train + norm_step).astype(jnp.bfloat16)
    return serving_gate, serving_up, factor_gate, factor_up, serve_norm, whole_gate, whole_up
```

```python
import functools
import math

import jax
import jax.numpy as jnp
from jax import lax
from jax.experimental import pallas as pl
from jax.experimental.pallas import tpu as pltpu
from jax.sharding import PartitionSpec as P

MESH = pl.DeviceIdType.MESH
keep_rate = 0.7


def grid_of(n_shard):
    chips = n_shard // 2
    nx = math.isqrt(chips)
    while chips % nx:
        nx -= 1
    return chips // nx, nx


def kernel(
    n_shard, n_model, ny, nx, pieces, strip,
    weight_gate, smooth_gate, weight_up, smooth_up, norm_train, norm_step,
    serve_gate, serve_up, factor_gate, factor_up, norm_all, whole_gate, whole_up,
    weights, smooths, peaks,
    load_sem, peak_send, peak_recv, norm_send, norm_recv, row_send, row_recv,
    x_send, y_send, pair_send, ring_recv, pair_recv,
):
    me = lax.axis_index("shard")
    col = lax.axis_index("model")
    core = lax.rem(me, 2)
    chip = me // 2
    xpos, ypos = lax.rem(chip, nx), chip // nx
    x_next = (ypos * nx + lax.rem(xpos + 1, nx)) * 2 + core
    y_next = (lax.rem(ypos + 1, ny) * nx + xpos) * 2 + core
    pair = chip * 2 + (1 - core)
    rows, cols = whole_gate.shape
    part = rows // pieces
    serves, wholes, factors = (serve_gate, serve_up), (whole_gate, whole_up), (factor_gate, factor_up)

    loads = {}
    for unit, (w_ref, s_ref) in enumerate(((weight_gate, smooth_gate), (weight_up, smooth_up))):
        for k in range(pieces):
            span = pl.ds(k * part, part)
            for which, (src, dst) in enumerate(((w_ref, weights), (s_ref, smooths))):
                copy = pltpu.make_async_copy(src.at[span], dst.at[unit, span], load_sem.at[unit, k, which])
                copy.start()
                loads[unit, k, which] = copy

    barrier = pltpu.get_barrier_semaphore()
    for d in range(1, n_shard):
        pl.semaphore_signal(barrier, inc=1, device_id=(lax.rem(me + d, n_shard), col), device_id_type=MESH)
    for d in range(1, n_model):
        pl.semaphore_signal(barrier, inc=1, device_id=(me, lax.rem(col + d, n_model)), device_id_type=MESH)

    per = norm_train.shape[1]
    norm_all[me, col, :, 0:per] = norm_train[...] + norm_step[...]

    def average(unit):
        top = jnp.zeros((8, cols), jnp.float32)
        for k in range(pieces):
            loads[unit, k, 0].wait()
            loads[unit, k, 1].wait()

            def step(i, top):
                span = pl.ds(pl.multiple_of(k * part + i * 8, 8), 8)
                value = keep_rate * smooths[unit, span, :] + (1.0 - keep_rate) * weights[unit, span, :]
                wholes[unit][span, :] = value
                return jnp.maximum(top, jnp.abs(value))

            top = lax.fori_loop(0, part // 8, step, top)
        peaks[unit, me] = jnp.max(top, axis=0, keepdims=True)

    def send_peaks(unit):
        copies = []
        for d in range(1, n_shard):
            copy = pltpu.make_async_remote_copy(
                src_ref=peaks.at[unit, me], dst_ref=peaks.at[unit, me],
                send_sem=peak_send.at[unit, d - 1], recv_sem=peak_recv.at[unit, d - 1],
                device_id=(lax.rem(me + d, n_shard), col), device_id_type=MESH,
            )
            copy.start()
            copies.append(copy)
        return copies

    average(0)
    pl.semaphore_wait(barrier, n_shard + n_model - 2)
    peak_copies = [send_peaks(0)]
    norm_copies = []
    for d in range(1, n_model):
        copy = pltpu.make_async_remote_copy(
            src_ref=norm_all.at[me, col], dst_ref=norm_all.at[me, col],
            send_sem=norm_send.at[d - 1], recv_sem=norm_recv.at[d - 1],
            device_id=(me, lax.rem(col + d, n_model)), device_id_type=MESH,
        )
        copy.start()
        norm_copies.append(copy)
    average(1)
    peak_copies.append(send_peaks(1))

    def place(dy, dx, k):
        owner = (lax.rem(ypos - dy + ny, ny) * nx + lax.rem(xpos - dx + nx, nx)) * 2
        return owner, k

    def piece_of(unit, dy, dx, k, side):
        owner = (lax.rem(ypos - dy + ny, ny) * nx + lax.rem(xpos - dx + nx, nx)) * 2 + side
        return serves[unit].at[pl.ds(pl.multiple_of(owner * rows + k * part, part), part)]

    sent = []

    def start(unit, dy, dx, k, device, send_sem, recv_sem):
        ref = piece_of(unit, dy, dx, k, core)
        copy = pltpu.make_async_remote_copy(
            src_ref=ref, dst_ref=ref, send_sem=send_sem, recv_sem=recv_sem,
            device_id=(device, col), device_id_type=MESH,
        )
        copy.start()
        sent.append(copy)

    def forward(unit, dy, dx, k):
        to_x = dx < nx - 1 and (unit == 1 or dy == 0)
        to_y = dy < ny - 1 and (unit == 0 or dx == 0)
        if to_x:
            start(unit, dy, dx, k, x_next, x_send.at[unit, dy, dx, k], ring_recv.at[unit, dy, dx + 1, k])
        if to_y:
            start(unit, dy, dx, k, y_next, y_send.at[unit, dy, dx, k], ring_recv.at[unit, dy + 1, dx, k])
        start(unit, dy, dx, k, pair, pair_send.at[unit, dy, dx, k], pair_recv.at[unit, dy, dx, k])

    def arrived(unit, dy, dx, k):
        ref = piece_of(unit, dy, dx, k, core)
        pltpu.make_async_copy(ref, ref, ring_recv.at[unit, dy, dx, k]).wait()

    for unit in range(2):
        for copy in peak_copies[unit]:
            copy.wait_recv()
        factor = peaks[unit, 0]
        for d in range(1, n_shard):
            factor = jnp.maximum(factor, peaks[unit, d])
        factors[unit][...] = factor
        for k in range(pieces):

            def narrow(i, carry):
                at = k * part + i * strip
                value = wholes[unit][pl.ds(pl.multiple_of(at, strip), strip), :] / factors[unit][...]
                serves[unit][pl.ds(pl.multiple_of(me * rows + at, strip), strip), :] = value.astype(jnp.bfloat16)
                return carry

            lax.fori_loop(0, part // strip, narrow, 0)
            if k:
                forward(unit, 0, 0, k - 1)
        if unit == 0:
            last = (0, 0, 0, pieces - 1)
        if unit == 0:
            for copy in norm_copies:
                copy.wait_recv()
            forward(*last)
    row_copies = []
    for d in range(1, n_shard):
        copy = pltpu.make_async_remote_copy(
            src_ref=norm_all.at[me], dst_ref=norm_all.at[me],
            send_sem=row_send.at[d - 1], recv_sem=row_recv.at[d - 1],
            device_id=(lax.rem(me + d, n_shard), col), device_id_type=MESH,
        )
        copy.start()
        row_copies.append(copy)
    forward(1, 0, 0, pieces - 1)

    for distance in range(1, ny + nx - 1):
        for unit in range(2):
            for k in range(pieces):
                for dy in range(ny):
                    dx = distance - dy
                    if 0 <= dx < nx:
                        arrived(unit, dy, dx, k)
                        forward(unit, dy, dx, k)

    for unit in range(2):
        for dy in range(ny):
            for dx in range(nx):
                for k in range(pieces):
                    ref = piece_of(unit, dy, dx, k, 1 - core)
                    pltpu.make_async_copy(ref, ref, pair_recv.at[unit, dy, dx, k]).wait()
    for copy in sent + peak_copies[0] + peak_copies[1] + norm_copies + row_copies:
        copy.wait_send()
    for copy in row_copies:
        copy.wait_recv()


def store_kernel(*refs):
    half = len(refs) // 2
    copies = []
    for i, (src, dst) in enumerate(zip(refs[:half], refs[half:-1])):
        copy = pltpu.make_async_copy(src, dst, refs[-1].at[i])
        copy.start()
        copies.append(copy)
    for copy in copies:
        copy.wait()


def store(arrays):
    hbm = pl.BlockSpec(memory_space=pltpu.HBM)
    return pl.pallas_call(
        store_kernel,
        out_shape=tuple(pltpu.HBM(a.shape, a.dtype) for a in arrays),
        in_specs=[pl.BlockSpec(memory_space=pltpu.VMEM)] * len(arrays),
        out_specs=(hbm,) * len(arrays),
        scratch_shapes=[pltpu.SemaphoreType.DMA((len(arrays),))],
        compiler_params=pltpu.CompilerParams(vmem_limit_bytes=1024 * 1024),
    )(*(pltpu.with_memory_space_constraint(a, pltpu.VMEM) for a in arrays))


def solution(mesh):
    n_shard, n_model = mesh.shape["shard"], mesh.shape["model"]
    ny, nx = grid_of(n_shard)
    pieces = max(1, 16 // (ny * nx))

    def body(weight_gate, smooth_gate, weight_up, smooth_up, norm_train, norm_step):
        rows, cols = weight_gate.shape
        per = norm_train.shape[0]
        wide = -(-per // 128) * 128
        vmem = pl.BlockSpec(memory_space=pltpu.VMEM)
        hbm = pl.BlockSpec(memory_space=pltpu.HBM)
        dma = pltpu.SemaphoreType.DMA
        full = (n_shard * rows, cols)
        landed = pl.pallas_call(
            functools.partial(kernel, n_shard, n_model, ny, nx, pieces, 16),
            out_shape=(
                pltpu.VMEM(full, jnp.bfloat16),
                pltpu.VMEM(full, jnp.bfloat16),
                pltpu.VMEM((1, cols), jnp.float32),
                pltpu.VMEM((1, cols), jnp.float32),
                pltpu.VMEM((n_shard, n_model, 1, wide), jnp.float32),
                pltpu.VMEM((rows, cols), jnp.float32),
                pltpu.VMEM((rows, cols), jnp.float32),
            ),
            in_specs=[hbm, hbm, hbm, hbm, vmem, vmem],
            out_specs=(vmem,) * 7,
            scratch_shapes=[
                pltpu.VMEM((2, rows, cols), jnp.float32),
                pltpu.VMEM((2, rows, cols), jnp.float32),
                pltpu.VMEM((2, n_shard, 1, cols), jnp.float32),
                dma((2, pieces, 2)),
                dma((2, n_shard)),
                dma((2, n_shard)),
                dma((n_model,)),
                dma((n_model,)),
                dma((n_shard,)),
                dma((n_shard,)),
                dma((2, ny, nx, pieces)),
                dma((2, ny, nx, pieces)),
                dma((2, ny, nx, pieces)),
                dma((2, ny, nx, pieces)),
                dma((2, ny, nx, pieces)),
            ],
            compiler_params=pltpu.CompilerParams(
                collective_id=0, has_side_effects=True, vmem_limit_bytes=20 * 1024 * 1024
            ),
        )(
            *(pltpu.with_memory_space_constraint(a, pltpu.HBM) for a in (weight_gate, smooth_gate, weight_up, smooth_up)),
            norm_train[None], norm_step[None],
        )
        serve_gate, serve_up, factor_gate, factor_up, norm_all, whole_gate, whole_up = store(landed)
        serve_norm = norm_all[:, :, 0, :per].reshape(-1).astype(jnp.bfloat16)
        return (
            serve_gate, serve_up, factor_gate.reshape(-1), factor_up.reshape(-1),
            serve_norm, whole_gate, whole_up,
        )

    in_specs = (P("shard", "model"),) * 4 + (P(("shard", "model")),) * 2
    out_specs = (
        P(None, "model"),
        P(None, "model"),
        P("model"),
        P("model"),
        P(),
        P("shard", "model"),
        P("shard", "model"),
    )
    return jax.shard_map(body, mesh=mesh, in_specs=in_specs, out_specs=out_specs, check_vma=False)
```

```python
import functools
import math

import jax
import jax.numpy as jnp
from jax import lax
from jax.experimental import pallas as pl
from jax.experimental.pallas import tpu as pltpu
from jax.sharding import PartitionSpec as P

MESH = pl.DeviceIdType.MESH
keep_rate = 0.7


def grid_of(n_shard):
    chips = n_shard // 2
    nx = math.isqrt(chips)
    while chips % nx:
        nx -= 1
    return chips // nx, nx


def kernel(
    n_shard, n_model, ny, nx, pieces,
    weight_gate, smooth_gate, weight_up, smooth_up, norm_train, norm_step,
    serve_gate, serve_up, factor_gate, factor_up, norm_all, whole_gate, whole_up,
    weights, smooths, peaks, norm_in,
    load_sem, norm_load, peak_send, peak_recv, norm_send, norm_recv, row_send, row_recv,
    x_send, y_send, pair_send, ring_recv, pair_recv,
):
    me = lax.axis_index("shard")
    col = lax.axis_index("model")
    core = lax.rem(me, 2)
    chip = me // 2
    xpos, ypos = lax.rem(chip, nx), chip // nx
    x_next = (ypos * nx + lax.rem(xpos + 1, nx)) * 2 + core
    y_next = (lax.rem(ypos + 1, ny) * nx + xpos) * 2 + core
    pair = chip * 2 + (1 - core)
    rows, cols = whole_gate.shape
    part = cols // pieces
    serves, wholes, factors = (serve_gate, serve_up), (whole_gate, whole_up), (factor_gate, factor_up)

    norm_loads = [
        pltpu.make_async_copy(src, norm_in.at[i], norm_load.at[i]) for i, src in enumerate((norm_train, norm_step))
    ]
    for copy in norm_loads:
        copy.start()
    loads = {}
    for unit, (w_ref, s_ref) in enumerate(((weight_gate, smooth_gate), (weight_up, smooth_up))):
        for k in sorted(range(pieces), key=lambda k: k % max(1, pieces // 2)):
            span = pl.ds(k * part, part)
            for which, (src, dst) in enumerate(((w_ref, weights), (s_ref, smooths))):
                copy = pltpu.make_async_copy(src.at[:, span], dst.at[unit, :, span], load_sem.at[unit, k, which])
                copy.start()
                loads[unit, k, which] = copy

    barrier = pltpu.get_barrier_semaphore()
    for d in range(1, n_shard):
        pl.semaphore_signal(barrier, inc=1, device_id=(lax.rem(me + d, n_shard), col), device_id_type=MESH)
    for d in range(1, n_model):
        pl.semaphore_signal(barrier, inc=1, device_id=(me, lax.rem(col + d, n_model)), device_id_type=MESH)

    per = norm_train.shape[1]
    for copy in norm_loads:
        copy.wait()
    norm_all[me, col, :, 0:per] = norm_in[0] + norm_in[1]

    def average(unit, k):
        for which in range(2):
            loads[unit, k, which].wait()
        across = pl.ds(k * part, part)

        def step(i, top):
            span = pl.ds(pl.multiple_of(i * 8, 8), 8)
            value = keep_rate * smooths[unit, span, across] + (1.0 - keep_rate) * weights[unit, span, across]
            wholes[unit][span, across] = value
            return jnp.maximum(top, jnp.abs(value))

        top = lax.fori_loop(0, rows // 8, step, jnp.zeros((8, part), jnp.float32), unroll=4)
        peaks[unit, k, me] = jnp.max(top, axis=0, keepdims=True)

    def send_peaks(unit, k):
        copies = []
        for d in range(1, n_shard):
            copy = pltpu.make_async_remote_copy(
                src_ref=peaks.at[unit, k, me], dst_ref=peaks.at[unit, k, me],
                send_sem=peak_send.at[unit, k, d - 1], recv_sem=peak_recv.at[unit, k, d - 1],
                device_id=(lax.rem(me + d, n_shard), col), device_id_type=MESH,
            )
            copy.start()
            copies.append(copy)
        return copies

    order = [(unit, k) for unit in range(2) for k in sorted(range(pieces), key=lambda k: k % max(1, pieces // 2))]
    peak_copies = {}
    norm_copies = []
    for n, (unit, k) in enumerate(order):
        average(unit, k)
        if n == 0:
            pl.semaphore_wait(barrier, n_shard + n_model - 2)
        peak_copies[unit, k] = send_peaks(unit, k)
    for d in range(1, n_model):
        copy = pltpu.make_async_remote_copy(
            src_ref=norm_all.at[me, col], dst_ref=norm_all.at[me, col],
            send_sem=norm_send.at[d - 1], recv_sem=norm_recv.at[d - 1],
            device_id=(me, lax.rem(col + d, n_model)), device_id_type=MESH,
        )
        copy.start()
        norm_copies.append(copy)

    def piece_of(unit, dy, dx, k, side):
        owner = (lax.rem(ypos - dy + ny, ny) * nx + lax.rem(xpos - dx + nx, nx)) * 2 + side
        return serves[unit].at[k, pl.ds(pl.multiple_of(owner * rows, rows), rows)]

    sent = []

    def start(unit, dy, dx, k, device, send_sem, recv_sem):
        ref = piece_of(unit, dy, dx, k, core)
        copy = pltpu.make_async_remote_copy(
            src_ref=ref, dst_ref=ref, send_sem=send_sem, recv_sem=recv_sem,
            device_id=(device, col), device_id_type=MESH,
        )
        copy.start()
        sent.append(copy)

    def along_x_first(unit, k):
        return 2 * k < pieces if pieces > 1 else unit == 0

    def to_x(unit, dy, dx, k):
        if dx < nx - 1 and (dy == 0 or not along_x_first(unit, k)):
            start(unit, dy, dx, k, x_next, x_send.at[unit, dy, dx, k], ring_recv.at[unit, dy, dx + 1, k])

    def to_y(unit, dy, dx, k):
        if dy < ny - 1 and (dx == 0 or along_x_first(unit, k)):
            start(unit, dy, dx, k, y_next, y_send.at[unit, dy, dx, k], ring_recv.at[unit, dy + 1, dx, k])

    def to_pair(unit, dy, dx, k):
        start(unit, dy, dx, k, pair, pair_send.at[unit, dy, dx, k], pair_recv.at[unit, dy, dx, k])

    def arrived(unit, dy, dx, k):
        ref = piece_of(unit, dy, dx, k, core)
        pltpu.make_async_copy(ref, ref, ring_recv.at[unit, dy, dx, k]).wait()

    def first_way(unit, k):
        (to_x if along_x_first(unit, k) else to_y)(unit, 0, 0, k)

    before = None
    for unit, k in order:
        across = pl.ds(k * part, part)
        for copy in peak_copies[unit, k]:
            copy.wait_recv()
        factor = peaks[unit, k, 0]
        for d in range(1, n_shard):
            factor = jnp.maximum(factor, peaks[unit, k, d])
        factors[unit][:, across] = factor
        if before:
            first_way(*before)

        def narrow(i, carry):
            at = i * 16
            value = wholes[unit][pl.ds(pl.multiple_of(at, 16), 16), across] / factors[unit][:, across]
            serves[unit][k, pl.ds(pl.multiple_of(me * rows + at, 16), 16)] = value.astype(jnp.bfloat16)
            return carry

        lax.fori_loop(0, rows // 16, narrow, 0, unroll=2)
        before = (unit, k)
    for copy in norm_copies:
        copy.wait_recv()
    row_copies = []
    for d in range(1, n_shard):
        copy = pltpu.make_async_remote_copy(
            src_ref=norm_all.at[me], dst_ref=norm_all.at[me],
            send_sem=row_send.at[d - 1], recv_sem=row_recv.at[d - 1],
            device_id=(lax.rem(me + d, n_shard), col), device_id_type=MESH,
        )
        copy.start()
        row_copies.append(copy)
    first_way(*before)
    for unit, k in order:
        (to_y if along_x_first(unit, k) else to_x)(unit, 0, 0, k)
    for unit, k in order:
        to_pair(unit, 0, 0, k)

    for distance in range(1, ny + nx - 1):
        for own_way in (True, False):
            for unit, k in order:
                for dy in range(ny):
                    dx = distance - dy
                    straight = (dy if along_x_first(unit, k) else dx) == 0
                    if 0 <= dx < nx and straight == own_way:
                        arrived(unit, dy, dx, k)
                        to_x(unit, dy, dx, k)
                        to_y(unit, dy, dx, k)
                        to_pair(unit, dy, dx, k)

    for unit in range(2):
        for dy in range(ny):
            for dx in range(nx):
                for k in range(pieces):
                    ref = piece_of(unit, dy, dx, k, 1 - core)
                    pltpu.make_async_copy(ref, ref, pair_recv.at[unit, dy, dx, k]).wait()
    for copy in sent + sum(peak_copies.values(), []) + norm_copies + row_copies:
        copy.wait_send()
    for copy in row_copies:
        copy.wait_recv()


def store_kernel(count, *refs):
    copies = []

    def move(src, dst):
        copies.append(pltpu.make_async_copy(src, dst, refs[-1].at[len(copies)]))
        copies[-1].start()

    for src, dst in zip(refs[:count], refs[count:-1]):
        if src.shape == dst.shape:
            move(src, dst)
            continue
        pieces, rows, part = src.shape
        for k in range(pieces):
            for half in range(2):
                span = pl.ds(half * (rows // 2), rows // 2)
                move(src.at[k, span], dst.at[span, pl.ds(k * part, part)])
    for copy in copies:
        copy.wait()


def store(arrays, shapes):
    hbm = pl.BlockSpec(memory_space=pltpu.HBM)
    return pl.pallas_call(
        functools.partial(store_kernel, len(arrays)),
        out_shape=tuple(pltpu.HBM(shape, a.dtype) for a, shape in zip(arrays, shapes)),
        in_specs=[pl.BlockSpec(memory_space=pltpu.VMEM)] * len(arrays),
        out_specs=(hbm,) * len(arrays),
        scratch_shapes=[pltpu.SemaphoreType.DMA((len(arrays) + 4 * arrays[0].shape[0],))],
        compiler_params=pltpu.CompilerParams(vmem_limit_bytes=1024 * 1024),
    )(*(pltpu.with_memory_space_constraint(a, pltpu.VMEM) for a in arrays))


def solution(mesh):
    n_shard, n_model = mesh.shape["shard"], mesh.shape["model"]
    ny, nx = grid_of(n_shard)

    def body(weight_gate, smooth_gate, weight_up, smooth_up, norm_train, norm_step):
        rows, cols = weight_gate.shape
        per = norm_train.shape[0]
        pieces = math.gcd(max(1, 16 // (ny * nx)), cols // 128)
        wide = -(-per // 128) * 128
        vmem = pl.BlockSpec(memory_space=pltpu.VMEM)
        hbm = pl.BlockSpec(memory_space=pltpu.HBM)
        dma = pltpu.SemaphoreType.DMA
        full = (pieces, n_shard * rows, cols // pieces)
        landed = pl.pallas_call(
            functools.partial(kernel, n_shard, n_model, ny, nx, pieces),
            out_shape=(
                pltpu.VMEM(full, jnp.bfloat16),
                pltpu.VMEM(full, jnp.bfloat16),
                pltpu.VMEM((1, cols), jnp.float32),
                pltpu.VMEM((1, cols), jnp.float32),
                pltpu.VMEM((n_shard, n_model, 1, wide), jnp.float32),
                pltpu.VMEM((rows, cols), jnp.float32),
                pltpu.VMEM((rows, cols), jnp.float32),
            ),
            in_specs=[hbm] * 6,
            out_specs=(vmem,) * 7,
            scratch_shapes=[
                pltpu.VMEM((2, rows, cols), jnp.float32),
                pltpu.VMEM((2, rows, cols), jnp.float32),
                pltpu.VMEM((2, pieces, n_shard, 1, cols // pieces), jnp.float32),
                pltpu.VMEM((2, 1, per), jnp.float32),
                dma((2, pieces, 2)),
                dma((2,)),
                dma((2, pieces, n_shard)),
                dma((2, pieces, n_shard)),
                dma((n_model,)),
                dma((n_model,)),
                dma((n_shard,)),
                dma((n_shard,)),
                dma((2, ny, nx, pieces)),
                dma((2, ny, nx, pieces)),
                dma((2, ny, nx, pieces)),
                dma((2, ny, nx, pieces)),
                dma((2, ny, nx, pieces)),
            ],
            compiler_params=pltpu.CompilerParams(
                collective_id=0, has_side_effects=True, vmem_limit_bytes=20 * 1024 * 1024
            ),
        )(
            *(
                pltpu.with_memory_space_constraint(a, pltpu.HBM)
                for a in (weight_gate, smooth_gate, weight_up, smooth_up, norm_train[None], norm_step[None])
            ),
        )
        serve_gate, serve_up, factor_gate, factor_up, norm_all, whole_gate, whole_up = store(
            landed, ((n_shard * rows, cols),) * 2 + tuple(a.shape for a in landed[2:])
        )
        serve_norm = norm_all[:, :, 0, :per].reshape(-1).astype(jnp.bfloat16)
        return (
            serve_gate, serve_up, factor_gate.reshape(-1), factor_up.reshape(-1),
            serve_norm, whole_gate, whole_up,
        )

    in_specs = (P("shard", "model"),) * 4 + (P(("shard", "model")),) * 2
    out_specs = (
        P(None, "model"),
        P(None, "model"),
        P("model"),
        P("model"),
        P(),
        P("shard", "model"),
        P("shard", "model"),
    )
    return jax.shard_map(body, mesh=mesh, in_specs=in_specs, out_specs=out_specs, check_vma=False)
```
